16 devices in a mesh: dp: 1, tp: 16 (over x, y, z, core).
Axes of the slice: x: 2, y: 2, z: 2, core: 2. Of those that a mesh axis runs over, the one named last changes fastest.
Arguments:
- x: bfloat16 [2048, 8192], P('dp')
- w_gate: bfloat16 [8192, 32768], P(None, 'tp')
- w_up: bfloat16 [8192, 32768], P(None, 'tp')
- w_down: bfloat16 [32768, 8192], P('tp')
Outputs:
- output: bfloat16 [2048, 8192], P('dp')
All inputs are finite; a program needn't handle non-finite values.
Results may differ from the reference program's by a relative error of at most 0.016.
Values are sent between devices in bfloat16 or wider.
A program may use at most 2 GiB of HBM per device.

```python
import jax
import jax.numpy as jnp

ROWS = 2048
D = 8192
FF = 32768


def setup_inputs(seed: int = 0, part: int = 0) -> dict:
    kx, kg, ku, kd = jax.random.split(jax.random.key(seed), 4)
    drawn = {
        "x": jax.random.normal(jax.random.fold_in(kx, part), (ROWS, D), jnp.float32),
        "w_gate": jax.random.normal(kg, (D, FF), jnp.float32) * D**-0.5,
        "w_up": jax.random.normal(ku, (D, FF), jnp.float32) * D**-0.5,
        "w_down": jax.random.normal(kd, (FF, D), jnp.float32) * FF**-0.5,
    }
    return {k: v.astype(jnp.bfloat16) for k, v in drawn.items()}


def reference(x, w_gate, w_up, w_down):
    gate = jnp.dot(x, w_gate, preferred_element_type=jnp.float32)
    up = jnp.dot(x, w_up, preferred_element_type=jnp.float32)
    hidden = (jax.nn.silu(gate) * up).astype(jnp.bfloat16)
    return jnp.dot(hidden, w_down, preferred_element_type=jnp.float32).astype(jnp.bfloat16)
```

```python
import functools

import jax
import jax.numpy as jnp
from jax import lax
from jax.experimental import pallas as pl
from jax.experimental.pallas import tpu as pltpu
from jax.sharding import PartitionSpec as P

MESH = pl.DeviceIdType.MESH
CHUNK = 512
TILES = 8
SLOTS = 8
KEEP = 3

EVENTS = (
    ("gather_core_wait", 7, 0),
    ("gather_core", 6, 1),
    ("gather3", 5, 0),
    ("gather2", 4, 0),
    ("gather1", 3, 1),
    ("sum3", 2, 2),
    ("sum2", 1, 2),
)


def kernel(
    x_ref, gate_ref, up_ref, down_ref, y_ref, other_ref,
    xb, gb, ub, db, hidden, gated,
    part, send1, keep2, send2, keep3, send3, final, recv1, recv2, recv3,
    load_sem, x_sem, down_sem, hid_send, hid_recv, other_send, other_recv, local_sem, send_sem, recv_sem,
):
    rows, depth = x_ref.shape
    width = gate_ref.shape[1]
    half = depth // 2
    tile, group = width // TILES, half // TILES
    chunks = rows // CHUNK
    n = chunks * TILES
    me = lax.axis_index("tp")
    core = lax.rem(me, 2)
    partner = me + 1 - 2 * core

    def to(device):
        return {"tp": device}

    def remote(src, dst, send, recv, device):
        return pltpu.make_async_remote_copy(
            src_ref=src, dst_ref=dst, send_sem=send, recv_sem=recv, device_id=to(device), device_id_type=MESH
        )

    def axis(d):
        d = lax.rem(d, 3)
        mask = 2 + d + d * d
        bit = lax.rem(me // mask, 2)
        return bit, me + mask * (1 - 2 * bit)

    barrier = pltpu.get_barrier_semaphore()
    for device in (partner, axis(0)[1], axis(1)[1], axis(2)[1]):
        pl.semaphore_signal(barrier, inc=1, device_id=to(device), device_id_type=MESH)
    pl.semaphore_wait(barrier, 4)

    def load_x(c):
        slot = lax.rem(c, 2)
        return pltpu.make_async_copy(
            x_ref.at[pl.ds(pl.multiple_of(c * CHUNK, CHUNK), CHUNK)], xb.at[slot], x_sem.at[slot]
        )

    def columns(t, size):
        return pl.ds(pl.multiple_of(t * size, size), size)

    def load_gate(i):
        return pltpu.make_async_copy(gate_ref.at[:, columns(lax.rem(i, TILES), tile)], gb, load_sem.at[0])

    def load_up(i):
        return pltpu.make_async_copy(up_ref.at[:, columns(lax.rem(i, TILES), tile)], ub, load_sem.at[1])

    def load_down(g):
        j = lax.rem(g, TILES)
        mine = pl.ds(pl.multiple_of(core * half + j * group, group), group)
        return (
            pltpu.make_async_copy(down_ref.at[:, mine], db.at[pl.ds(0, width)], down_sem.at[0]),
            pltpu.make_async_copy(other_ref.at[:, columns(j, group)], db.at[pl.ds(width, width)], down_sem.at[1]),
        )

    theirs = pl.ds(pl.multiple_of((1 - core) * half, half), half)
    swap_down = remote(down_ref.at[:, theirs], other_ref, other_send, other_recv, partner)

    def swap_hidden(i):
        slot, t = lax.rem(i // TILES, 2), lax.rem(i, TILES)
        return remote(
            hidden.at[slot, :, columns(t, tile)],
            hidden.at[slot, :, pl.ds(pl.multiple_of(width + t * tile, tile), tile)],
            hid_send.at[slot, t], hid_recv.at[slot, t], partner,
        )

    class Group:
        def __init__(self, g):
            self.s, self.k = lax.rem(g, SLOTS), lax.rem(g, KEEP)
            rot = lax.rem(g, 3)
            (self.b1, self.n1), (self.b2, self.n2), (self.b3, self.n3) = axis(rot), axis(rot + 1), axis(rot + 2)
            self.r0 = (g // TILES) * CHUNK
            self.r1 = self.r0 + self.b1 * (CHUNK // 2)
            self.r2 = self.r1 + self.b2 * (CHUNK // 4)
            self.r3 = self.r2 + self.b3 * (CHUNK // 8)
            self.cols = pl.ds(pl.multiple_of(core * half + lax.rem(g, TILES) * group, group), group)

        def copy(self, stage, src, dst, device):
            return remote(src, dst, send_sem.at[stage, self.s], recv_sem.at[stage, self.s], device)

        def reduce1(self):
            return self.copy(0, send1.at[self.k], recv1.at[self.s], self.n1)

        def reduce2(self):
            return self.copy(1, send2.at[self.k], recv2.at[self.s], self.n2)

        def reduce3(self):
            return self.copy(2, send3.at[self.k], recv3.at[self.s], self.n3)

        def window(self, row, size):
            return y_ref.at[pl.ds(pl.multiple_of(row, size), size), self.cols]

        def local(self):
            return pltpu.make_async_copy(
                final.at[self.k], self.window(self.r3, CHUNK // 8), local_sem.at[self.s]
            )

        def gather1(self):
            return self.copy(3, final.at[self.k], self.window(self.r3, CHUNK // 8), self.n3)

        def gather2(self):
            w = self.window(self.r2, CHUNK // 4)
            return self.copy(4, w, w, self.n2)

        def gather3(self):
            w = self.window(self.r1, CHUNK // 2)
            return self.copy(5, w, w, self.n1)

        def gather_core(self):
            w = self.window(self.r0, CHUNK)
            return self.copy(6, w, w, partner)

    def rows_at(bit, size):
        return pl.ds(pl.multiple_of(bit * size, size), size)

    def sum1(g):
        q = Group(g)
        send1[q.k] = part[q.k, rows_at(1 - q.b1, CHUNK // 2)].astype(jnp.bfloat16)
        q.reduce1().start()

    def sum2(g):
        q = Group(g)
        size = CHUNK // 4
        q.reduce1().wait()
        for keep in (False, True):
            bit = q.b2 if keep else 1 - q.b2
            mine = part[q.k, pl.ds(pl.multiple_of(q.b1 * (CHUNK // 2) + bit * size, size), size)]
            total = mine + recv1[q.s, rows_at(bit, size)].astype(jnp.float32)
            if keep:
                keep2[q.k] = total
            else:
                send2[q.k] = total.astype(jnp.bfloat16)
                q.reduce2().start()

    def sum3(g):
        q = Group(g)
        size = CHUNK // 8
        q.reduce2().wait()
        for keep in (False, True):
            bit = q.b3 if keep else 1 - q.b3
            total = keep2[q.k, rows_at(bit, size)] + recv2[q.s, rows_at(bit, size)].astype(jnp.float32)
            if keep:
                keep3[q.k] = total
            else:
                send3[q.k] = total.astype(jnp.bfloat16)
                q.reduce3().start()

    def gather1(g):
        q = Group(g)
        q.reduce3().wait()
        final[q.k] = (keep3[q.k] + recv3[q.s].astype(jnp.float32)).astype(jnp.bfloat16)
        q.gather1().start()
        q.local().start()

    def gather2(g):
        q = Group(g)
        q.gather1().wait()
        q.local().wait()
        q.gather2().start()

    def gather3(g):
        q = Group(g)
        q.gather2().wait()
        q.gather3().start()

    def gather_core(g):
        q = Group(g)
        q.gather3().wait()
        q.gather_core().start()

    def gather_core_wait(g):
        Group(g).gather_core().wait()

    stages = dict(
        sum2=sum2, sum3=sum3, gather1=gather1, gather2=gather2, gather3=gather3,
        gather_core=gather_core, gather_core_wait=gather_core_wait,
    )

    def events(i, place):
        for name, delay, where in EVENTS:
            if where == place:
                g = i - TILES - delay
                pl.when((g >= 0) & (g < n))(functools.partial(stages[name], g))

    load_x(0).start()
    load_gate(0).start()
    load_up(0).start()

    def body(i, carry):
        slot, t = lax.rem(i // TILES, 2), lax.rem(i, TILES)
        g = i - TILES

        @pl.when(i < n)
        def _():
            pl.when(t == 0)(lambda: load_x(i // TILES).wait())
            load_gate(i).wait()
            gated[...] = jnp.dot(xb[slot], gb[...], preferred_element_type=jnp.float32)
            pl.when(i + 1 < n)(lambda: load_gate(i + 1).start())

        @pl.when(i == 0)
        def _():
            swap_down.start()
            if chunks > 1:
                load_x(1).start()

        events(i, 0)

        @pl.when((g >= 0) & (g < n))
        def _():
            @pl.when(lax.rem(g, TILES) == 0)
            def _():
                for t in range(TILES):
                    swap_hidden((g // TILES) * TILES + t).wait()

            for copy in load_down(g):
                copy.wait()
            part[lax.rem(g, KEEP)] = jnp.dot(
                hidden[lax.rem(g // TILES, 2)], db[...], preferred_element_type=jnp.float32
            )
            sum1(g)

        @pl.when(g == -1)
        def _():
            swap_down.wait()

        @pl.when((g >= -1) & (g < n - 1))
        def _():
            for copy in load_down(g + 1):
                copy.start()

        events(i, 1)

        @pl.when(i < n)
        def _():
            load_up(i).wait()
            up = jnp.dot(xb[slot], ub[...], preferred_element_type=jnp.float32)
            pl.when(i + 1 < n)(lambda: load_up(i + 1).start())
            hidden[slot, :, columns(t, tile)] = (jax.nn.silu(gated[...]) * up).astype(jnp.bfloat16)
            swap_hidden(i).start()
            pl.when((t == TILES - 1) & (i // TILES + 2 < chunks))(lambda: load_x(i // TILES + 2).start())

        events(i, 2)
        return carry

    lax.fori_loop(0, n + TILES + 1 + max(e[1] for e in EVENTS), body, 0)


def block(x, w_gate, w_up, w_down):
    rows, depth = x.shape
    width = w_gate.shape[1]
    half = depth // 2
    tile, group = width // TILES, half // TILES
    b16, f32 = jnp.bfloat16, jnp.float32
    dma = pltpu.SemaphoreType.DMA
    flops = 6 * rows * depth * width
    y, _ = pl.pallas_call(
        kernel,
        out_shape=(jax.ShapeDtypeStruct((rows, depth), b16), jax.ShapeDtypeStruct((width, half), b16)),
        in_specs=[pl.BlockSpec(memory_space=pl.ANY)] * 4,
        out_specs=(pl.BlockSpec(memory_space=pl.ANY),) * 2,
        scratch_shapes=[
            pltpu.VMEM((2, CHUNK, depth), b16),
            pltpu.VMEM((depth, tile), b16),
            pltpu.VMEM((depth, tile), b16),
            pltpu.VMEM((2 * width, group), b16),
            pltpu.VMEM((2, CHUNK, 2 * width), b16),
            pltpu.VMEM((CHUNK, tile), f32),
            pltpu.VMEM((KEEP, CHUNK, group), f32),
            pltpu.VMEM((KEEP, CHUNK // 2, group), b16),
            pltpu.VMEM((KEEP, CHUNK // 4, group), f32),
            pltpu.VMEM((KEEP, CHUNK // 4, group), b16),
            pltpu.VMEM((KEEP, CHUNK // 8, group), f32),
            pltpu.VMEM((KEEP, CHUNK // 8, group), b16),
            pltpu.VMEM((KEEP, CHUNK // 8, group), b16),
            pltpu.VMEM((SLOTS, CHUNK // 2, group), b16),
            pltpu.VMEM((SLOTS, CHUNK // 4, group), b16),
            pltpu.VMEM((SLOTS, CHUNK // 8, group), b16),
            dma((2,)), dma((2,)), dma((2,)), dma((2, TILES)), dma((2, TILES)), dma, dma, dma((SLOTS,)),
            dma((7, SLOTS)), dma((7, SLOTS)),
        ],
        compiler_params=pltpu.CompilerParams(
            collective_id=0, has_side_effects=True, vmem_limit_bytes=64_000_000
        ),
        cost_estimate=pl.CostEstimate(flops=flops, bytes_accessed=8 * depth * width, transcendentals=rows * width),
    )(x, w_gate, w_up, w_down)
    return y


def solution(mesh):
    return jax.shard_map(
        block,
        mesh=mesh,
        in_specs=(P("dp", None), P(None, "tp"), P(None, "tp"), P("tp", None)),
        out_specs=P("dp", None),
        check_vma=False,
    )
```

```python
import functools

import jax
import jax.numpy as jnp
from jax import lax
from jax.experimental import pallas as pl
from jax.experimental.pallas import tpu as pltpu
from jax.sharding import PartitionSpec as P

MESH = pl.DeviceIdType.MESH
SIZES = (512, 384, 384, 384, 384)
TILES = 8
SLOTS = 12
KEEP = 3
PARTS = ((0, 4),)
TURN = 1
SPLIT = 4

EVENTS = (
    ("gather_core_wait", 27, 0, 0, 22),
    ("gather_core", 11, 0, 0, 22),
    ("gather_core", 23, 0, 29, 40),
    ("gather3", 14, 0, 29, 40),
    ("gather2", 6, 0, 22, 29),
    ("gather1", 5, 0, 0, 29),
    ("gather1", 8, 0, 29, 40),
    ("sum3", 4, 0, 0, 22),
    ("sum3", 5, 0, 29, 40),
    ("sum2", 2, 0, 22, 29),
    ("gather_core_wait", 26, 1, 22, 29),
    ("gather_core_wait", 28, 1, 29, 40),
    ("gather_core", 11, 1, 22, 29),
    ("gather3", 8, 1, 0, 29),
    ("gather2", 6, 1, 0, 22),
    ("gather2", 10, 1, 29, 40),
    ("sum3", 3, 1, 22, 29),
    ("sum2", 2, 1, 0, 22),
    ("sum2", 2, 1, 29, 40),
)


def phases():
    runs, row = [], 0
    for c, size in enumerate(SIZES):
        if runs and runs[-1][2] == size:
            runs[-1][1] = c + 1
        else:
            runs.append([c, c + 1, size, row])
        row += size
    return runs


def kernel(
    x_ref, gate_ref, up_ref, down_ref, y_ref, other_ref,
    xb, gb, ub, db, hidden, gated,
    part, send1, keep2, send2, keep3, send3, final, recv1, recv2, recv3,
    load_sem, first_sem, x_sem, down_sem, hid_send, hid_recv, other_send, other_recv, local_sem, send_sem, recv_sem,
    core_send, core_recv,
):
    rows, depth = x_ref.shape
    width = gate_ref.shape[1]
    half = depth // 2
    tile, group = width // TILES, half // TILES
    chunks = len(SIZES)
    n = chunks * TILES
    parts = tuple((a * group // 4, b * group // 4) for a, b in PARTS)
    me = lax.axis_index("tp")
    core = lax.rem(me, 2)
    partner = me + 1 - 2 * core

    def to(device):
        return {"tp": device}

    def remote(src, dst, send, recv, device):
        return pltpu.make_async_remote_copy(
            src_ref=src, dst_ref=dst, send_sem=send, recv_sem=recv, device_id=to(device), device_id_type=MESH
        )

    def axis(d):
        d = lax.rem(d, 3)
        mask = 2 + d + d * d
        bit = lax.rem(me // mask, 2)
        return bit, me + mask * (1 - 2 * bit)

    barrier = pltpu.get_barrier_semaphore()
    for device in (partner, axis(0)[1], axis(1)[1], axis(2)[1]):
        pl.semaphore_signal(barrier, inc=1, device_id=to(device), device_id_type=MESH)
    pl.semaphore_wait(barrier, 4)

    def by_size(c, do):
        for first, last, size, row in phases():
            pl.when((c >= first) & (c < last))(functools.partial(do, size, row + (c - first) * size))

    def load_x(c):
        slot = lax.rem(c, 2)

        def copy(size, row):
            rows_ = pl.ds(pl.multiple_of(row, 128), size)
            return pltpu.make_async_copy(x_ref.at[rows_], xb.at[slot, pl.ds(0, size)], x_sem.at[slot])

        return copy

    def start_x(c):
        by_size(c, lambda size, row: load_x(c)(size, row).start())

    def first_loads():
        step = depth // SPLIT
        for k in range(SPLIT):
            cut = pl.ds(k * step, step)
            yield (
                pltpu.make_async_copy(
                    x_ref.at[pl.ds(0, SIZES[0]), cut], xb.at[0, pl.ds(0, SIZES[0]), cut], first_sem.at[0, k]
                ),
                pltpu.make_async_copy(gate_ref.at[cut, pl.ds(0, tile)], gb.at[0, cut], first_sem.at[1, k]),
            )

    def columns(t, size):
        return pl.ds(pl.multiple_of(t * size, size), size)

    def load_gate(i):
        return pltpu.make_async_copy(gate_ref.at[:, columns(lax.rem(i, TILES), tile)], gb.at[lax.rem(i, 2)], load_sem.at[0, lax.rem(i, 2)])

    def load_up(i):
        return pltpu.make_async_copy(up_ref.at[:, columns(lax.rem(i, TILES), tile)], ub.at[lax.rem(i, 2)], load_sem.at[1, lax.rem(i, 2)])

    def load_down(g):
        j = lax.rem(g, TILES)
        mine = pl.ds(pl.multiple_of(core * half + j * group, group), group)
        return (
            pltpu.make_async_copy(down_ref.at[:, mine], db.at[pl.ds(0, width)], down_sem.at[0]),
            pltpu.make_async_copy(other_ref.at[:, columns(j, group)], db.at[pl.ds(width, width)], down_sem.at[1]),
        )

    theirs = pl.ds(pl.multiple_of((1 - core) * half, half), half)
    swap_down = remote(down_ref.at[:, theirs], other_ref, other_send, other_recv, partner)

    def swap_hidden(i, size):
        slot, t = lax.rem(i // TILES, 2), lax.rem(i, TILES)
        return remote(
            hidden.at[slot, pl.ds(0, size), columns(t, tile)],
            hidden.at[slot, pl.ds(0, size), pl.ds(pl.multiple_of(width + t * tile, tile), tile)],
            hid_send.at[slot, t], hid_recv.at[slot, t], partner,
        )

    class Part:
        def __init__(self, g, size, row, p):
            self.p, self.size = p, size
            self.s, self.k = lax.rem(g, SLOTS), lax.rem(g, KEEP)
            (self.b1, self.n1), (self.b2, self.n2), (self.b3, self.n3) = (axis(TURN * g + p + d) for d in range(3))
            self.r1 = row + self.b1 * (size // 2)
            self.r2 = self.r1 + self.b2 * (size // 4)
            self.r3 = self.r2 + self.b3 * (size // 8)
            start, wide = parts[p]
            self.cut = pl.ds(start, wide)
            self.cols = pl.ds(pl.multiple_of(core * half + lax.rem(g, TILES) * group + start, 128), wide)

        def copy(self, stage, src, dst, device):
            return remote(src, dst, send_sem.at[stage, self.p, self.s], recv_sem.at[stage, self.p, self.s], device)

        def reduce(self, stage):
            rows_ = pl.ds(0, self.size >> stage)
            send = (send1, send2, send3)[stage - 1].at[self.k, rows_, self.cut]
            recv = (recv1, recv2, recv3)[stage - 1].at[self.s, rows_, self.cut]
            return self.copy(stage - 1, send, recv, (self.n1, self.n2, self.n3)[stage - 1])

        def window(self, row, size):
            return y_ref.at[pl.ds(pl.multiple_of(row, 16), size), self.cols]

        def final(self):
            return final.at[self.k, pl.ds(0, self.size // 8), self.cut]

        def local(self):
            return pltpu.make_async_copy(
                self.final(), self.window(self.r3, self.size // 8), local_sem.at[self.p, self.s]
            )

        def gather(self, stage):
            if stage == 1:
                return self.copy(3, self.final(), self.window(self.r3, self.size // 8), self.n3)
            if stage == 2:
                w, device = self.window(self.r2, self.size // 4), self.n2
            else:
                w, device = self.window(self.r1, self.size // 2), self.n1
            return self.copy(stage + 2, w, w, device)

    def each_part(do):
        def stage(g, size, row):
            for p in range(len(parts)):
                do(Part(g, size, row, p))

        return stage

    def rows_at(offset, size):
        return pl.ds(pl.multiple_of(offset, 16), size)

    @each_part
    def sum1(q):
        h = q.size // 2
        send1[q.k, 0:h, q.cut] = part[q.k, rows_at((1 - q.b1) * h, h), q.cut].astype(jnp.bfloat16)
        q.reduce(1).start()

    @each_part
    def sum2(q):
        h = q.size // 4
        q.reduce(1).wait()
        for keep in (False, True):
            at = (q.b2 if keep else 1 - q.b2) * h
            total = part[q.k, rows_at(q.b1 * (q.size // 2) + at, h), q.cut] + recv1[
                q.s, rows_at(at, h), q.cut
            ].astype(jnp.float32)
            if keep:
                keep2[q.k, 0:h, q.cut] = total
            else:
                send2[q.k, 0:h, q.cut] = total.astype(jnp.bfloat16)
                q.reduce(2).start()

    @each_part
    def sum3(q):
        h = q.size // 8
        q.reduce(2).wait()
        for keep in (False, True):
            at = (q.b3 if keep else 1 - q.b3) * h
            total = keep2[q.k, rows_at(at, h), q.cut] + recv2[q.s, rows_at(at, h), q.cut].astype(jnp.float32)
            if keep:
                keep3[q.k, 0:h, q.cut] = total
            else:
                send3[q.k, 0:h, q.cut] = total.astype(jnp.bfloat16)
                q.reduce(3).start()

    @each_part
    def gather1(q):
        h = q.size // 8
        q.reduce(3).wait()
        total = keep3[q.k, 0:h, q.cut] + recv3[q.s, 0:h, q.cut].astype(jnp.float32)
        final[q.k, 0:h, q.cut] = total.astype(jnp.bfloat16)
        q.gather(1).start()
        q.local().start()

    @each_part
    def gather2(q):
        q.gather(1).wait()
        q.local().wait()
        q.gather(2).start()

    @each_part
    def gather3(q):
        q.gather(2).wait()
        q.gather(3).start()

    @each_part
    def gathered(q):
        q.gather(3).wait()

    def across(g, size, row):
        cols = pl.ds(pl.multiple_of(core * half + lax.rem(g, TILES) * group, group), group)
        w = y_ref.at[pl.ds(pl.multiple_of(row, 16), size), cols]
        return remote(w, w, core_send.at[g], core_recv.at[g], partner)

    def gather_core(g, size, row):
        gathered(g, size, row)
        across(g, size, row).start()

    def gather_core_wait(g, size, row):
        across(g, size, row).wait()

    stages = dict(
        sum2=sum2, sum3=sum3, gather1=gather1, gather2=gather2, gather3=gather3,
        gather_core=gather_core, gather_core_wait=gather_core_wait,
    )

    def events(i, place):
        for name, delay, where, first, last in EVENTS:
            if where == place:
                g = i - TILES - delay
                pl.when((g >= first) & (g < last))(
                    functools.partial(by_size, g // TILES, functools.partial(stages[name], g))
                )

    for pair in first_loads():
        for copy in pair:
            copy.start()
    load_up(0).start()

    def body(i, carry):
        slot, t = lax.rem(i // TILES, 2), lax.rem(i, TILES)
        g = i - TILES

        @pl.when(i + 1 < n)
        def _():
            load_gate(i + 1).start()
            load_up(i + 1).start()

        def activate(size, gate, up):
            hidden[slot, 0:size, columns(t, tile)] = (jax.nn.silu(gate) * up).astype(jnp.bfloat16)

        @pl.when(i == 0)
        def _():
            step, size = depth // SPLIT, SIZES[0]
            for k, pair in enumerate(first_loads()):
                for copy in pair:
                    copy.wait()
                cut = pl.ds(k * step, step)
                term = jnp.dot(xb[0, 0:size, cut], gb[0, cut], preferred_element_type=jnp.float32)
                gated[...] = term if k == 0 else gated[...] + term
            load_up(0).wait()
            activate(size, gated[...], jnp.dot(xb[0, 0:size], ub[0], preferred_element_type=jnp.float32))
            swap_down.start()
            if chunks > 1:
                start_x(1)

        @pl.when((i > 0) & (i < n))
        def _():
            load_gate(i).wait()
            load_up(i).wait()

            def dots(size, row):
                pl.when(t == 0)(lambda: load_x(i // TILES)(size, row).wait())
                gated[0:size] = jnp.dot(xb[slot, 0:size], gb[lax.rem(i, 2)], preferred_element_type=jnp.float32)
                up = jnp.dot(xb[slot, 0:size], ub[lax.rem(i, 2)], preferred_element_type=jnp.float32)
                activate(size, gated[0:size], up)

            by_size(i // TILES, dots)
            pl.when(t == TILES - 1)(lambda: start_x(i // TILES + 2))

        events(i, 0)
        @pl.when((g >= 0) & (g < n))
        def _():
            for copy in load_down(g):
                copy.wait()

            def dot(size, row):
                @pl.when(lax.rem(g, TILES) == 0)
                def _():
                    for t in range(TILES):
                        swap_hidden((g // TILES) * TILES + t, size).wait()

                part[lax.rem(g, KEEP), 0:size] = jnp.dot(
                    hidden[lax.rem(g // TILES, 2), 0:size], db[...], preferred_element_type=jnp.float32
                )
                sum1(g, size, row)

            by_size(g // TILES, dot)

        pl.when(g == -1)(lambda: swap_down.wait())

        @pl.when((g >= -1) & (g < n - 1))
        def _():
            for copy in load_down(g + 1):
                copy.start()

        pl.when(i < n)(lambda: by_size(i // TILES, lambda size, row: swap_hidden(i, size).start()))
        events(i, 1)
        return carry

    lax.fori_loop(0, n + TILES + 1 + max(e[1] for e in EVENTS), body, 0)


def block(x, w_gate, w_up, w_down):
    rows, depth = x.shape
    width = w_gate.shape[1]
    half = depth // 2
    tile, group, most = width // TILES, half // TILES, max(SIZES)
    b16, f32 = jnp.bfloat16, jnp.float32
    dma = pltpu.SemaphoreType.DMA
    flops = 6 * rows * depth * width
    y, _ = pl.pallas_call(
        kernel,
        out_shape=(jax.ShapeDtypeStruct((rows, depth), b16), jax.ShapeDtypeStruct((width, half), b16)),
        in_specs=[pl.BlockSpec(memory_space=pl.ANY)] * 4,
        out_specs=(pl.BlockSpec(memory_space=pl.ANY),) * 2,
        scratch_shapes=[
            pltpu.VMEM((2, most, depth), b16),
            pltpu.VMEM((2, depth, tile), b16),
            pltpu.VMEM((2, depth, tile), b16),
            pltpu.VMEM((2 * width, group), b16),
            pltpu.VMEM((2, most, 2 * width), b16),
            pltpu.VMEM((most, tile), f32),
            pltpu.VMEM((KEEP, most, group), f32),
            pltpu.VMEM((KEEP, most // 2, group), b16),
            pltpu.VMEM((KEEP, most // 4, group), f32),
            pltpu.VMEM((KEEP, most // 4, group), b16),
            pltpu.VMEM((KEEP, most // 8, group), f32),
            pltpu.VMEM((KEEP, most // 8, group), b16),
            pltpu.VMEM((KEEP, most // 8, group), b16),
            pltpu.VMEM((SLOTS, most // 2, group), b16),
            pltpu.VMEM((SLOTS, most // 4, group), b16),
            pltpu.VMEM((SLOTS, most // 8, group), b16),
            dma((2, 2)), dma((2, SPLIT)), dma((2,)), dma((2,)), dma((2, TILES)), dma((2, TILES)), dma, dma, dma((len(PARTS), SLOTS)),
            dma((6, len(PARTS), SLOTS)), dma((6, len(PARTS), SLOTS)), dma((len(SIZES) * TILES,)), dma((len(SIZES) * TILES,)),
        ],
        compiler_params=pltpu.CompilerParams(
            collective_id=0, has_side_effects=True, vmem_limit_bytes=67_000_000
        ),
        cost_estimate=pl.CostEstimate(flops=flops, bytes_accessed=8 * depth * width, transcendentals=rows * width),
    )(x, w_gate, w_up, w_down)
    return y


def solution(mesh):
    return jax.shard_map(
        block,
        mesh=mesh,
        in_specs=(P("dp", None), P(None, "tp"), P(None, "tp"), P("tp", None)),
        out_specs=P("dp", None),
        check_vma=False,
    )
```

```python
import functools

import jax
import jax.numpy as jnp
from jax import lax
from jax.experimental import pallas as pl
from jax.experimental.pallas import tpu as pltpu
from jax.sharding import PartitionSpec as P

MESH = pl.DeviceIdType.MESH
SIZES = (512, 384, 384, 384, 384)
TILES = 8
SLOTS = 12
KEEP = 3
PARTS = ((0, 4),)
TURN = 1
SPLIT = 4

EVENTS = (
    ("gather_core", 17, 0, 32, 40),
    ("gather3", 8, 0, 0, 32),
    ("gather1", 5, 0, 0, 40),
    ("sum3", 4, 0, 0, 2),
    ("sum2", 2, 0, 2, 40),
    ("gather_core_wait", 23, 1, 0, 2),
    ("gather_core_wait", 26, 1, 2, 32),
    ("gather_core_wait", 25, 1, 32, 40),
    ("gather_core", 11, 1, 0, 32),
    ("gather3", 9, 1, 32, 40),
    ("gather2", 6, 1, 0, 40),
    ("sum3", 3, 1, 2, 40),
    ("sum2", 2, 1, 0, 2),
)


def phases():
    runs, row = [], 0
    for c, size in enumerate(SIZES):
        if runs and runs[-1][2] == size:
            runs[-1][1] = c + 1
        else:
            runs.append([c, c + 1, size, row])
        row += size
    return runs


def kernel(
    x_ref, gate_ref, up_ref, down_ref, y_ref, other_ref,
    xb, gb, ub, db, hidden, gated,
    part, send1, keep2, send2, keep3, send3, final, recv1, recv2, recv3,
    load_sem, first_sem, x_sem, down_sem, hid_send, hid_recv, other_send, other_recv, local_sem, send_sem, recv_sem,
    core_send, core_recv,
):
    rows, depth = x_ref.shape
    width = gate_ref.shape[1]
    half = depth // 2
    tile, group = width // TILES, half // TILES
    chunks = len(SIZES)
    n = chunks * TILES
    parts = tuple((a * group // 4, b * group // 4) for a, b in PARTS)
    me = lax.axis_index("tp")
    core = lax.rem(me, 2)
    partner = me + 1 - 2 * core

    def to(device):
        return {"tp": device}

    def remote(src, dst, send, recv, device):
        return pltpu.make_async_remote_copy(
            src_ref=src, dst_ref=dst, send_sem=send, recv_sem=recv, device_id=to(device), device_id_type=MESH
        )

    def axis(d):
        d = lax.rem(d, 3)
        mask = 2 + d + d * d
        bit = lax.rem(me // mask, 2)
        return bit, me + mask * (1 - 2 * bit)

    barrier = pltpu.get_barrier_semaphore()
    for device in (partner, axis(0)[1], axis(1)[1], axis(2)[1]):
        pl.semaphore_signal(barrier, inc=1, device_id=to(device), device_id_type=MESH)
    pl.semaphore_wait(barrier, 4)

    def by_size(c, do):
        for first, last, size, row in phases():
            pl.when((c >= first) & (c < last))(functools.partial(do, size, row + (c - first) * size))

    def load_x(c):
        slot = lax.rem(c, 2)

        def copy(size, row):
            rows_ = pl.ds(pl.multiple_of(row, 128), size)
            return pltpu.make_async_copy(x_ref.at[rows_], xb.at[slot, pl.ds(0, size)], x_sem.at[slot])

        return copy

    def start_x(c):
        by_size(c, lambda size, row: load_x(c)(size, row).start())

    def first_loads():
        step = depth // SPLIT
        for k in range(SPLIT):
            cut = pl.ds(k * step, step)
            yield (
                pltpu.make_async_copy(
                    x_ref.at[pl.ds(0, SIZES[0]), cut], xb.at[0, pl.ds(0, SIZES[0]), cut], first_sem.at[0, k]
                ),
                pltpu.make_async_copy(gate_ref.at[cut, pl.ds(0, tile)], gb.at[0, cut], first_sem.at[1, k]),
            )

    def columns(t, size):
        return pl.ds(pl.multiple_of(t * size, size), size)

    def load_gate(i):
        return pltpu.make_async_copy(gate_ref.at[:, columns(lax.rem(i, TILES), tile)], gb.at[lax.rem(i, 2)], load_sem.at[0, lax.rem(i, 2)])

    def load_up(i):
        return pltpu.make_async_copy(up_ref.at[:, columns(lax.rem(i, TILES), tile)], ub.at[lax.rem(i, 2)], load_sem.at[1, lax.rem(i, 2)])

    def load_down(g):
        j, s = lax.rem(g, TILES), lax.rem(g, 2)
        mine = pl.ds(pl.multiple_of(core * half + j * group, group), group)
        return (
            pltpu.make_async_copy(down_ref.at[:, mine], db.at[s, pl.ds(0, width)], down_sem.at[0, s]),
            pltpu.make_async_copy(other_ref.at[:, columns(j, group)], db.at[s, pl.ds(width, width)], down_sem.at[1, s]),
        )

    theirs = pl.ds(pl.multiple_of((1 - core) * half, half), half)
    swap_down = remote(down_ref.at[:, theirs], other_ref, other_send, other_recv, partner)

    def swap_hidden(i, size):
        slot, t = lax.rem(i // TILES, 2), lax.rem(i, TILES)
        return remote(
            hidden.at[slot, pl.ds(0, size), columns(t, tile)],
            hidden.at[slot, pl.ds(0, size), pl.ds(pl.multiple_of(width + t * tile, tile), tile)],
            hid_send.at[slot, t], hid_recv.at[slot, t], partner,
        )

    class Part:
        def __init__(self, g, size, row, p):
            self.p, self.size = p, size
            self.s, self.k = lax.rem(g, SLOTS), lax.rem(g, KEEP)
            (self.b1, self.n1), (self.b2, self.n2), (self.b3, self.n3) = (axis(TURN * g + p + d) for d in range(3))
            self.r1 = row + self.b1 * (size // 2)
            self.r2 = self.r1 + self.b2 * (size // 4)
            self.r3 = self.r2 + self.b3 * (size // 8)
            start, wide = parts[p]
            self.cut = pl.ds(start, wide)
            self.cols = pl.ds(pl.multiple_of(core * half + lax.rem(g, TILES) * group + start, 128), wide)

        def copy(self, stage, src, dst, device):
            return remote(src, dst, send_sem.at[stage, self.p, self.s], recv_sem.at[stage, self.p, self.s], device)

        def reduce(self, stage):
            rows_ = pl.ds(0, self.size >> stage)
            send = (send1, send2, send3)[stage - 1].at[self.k, rows_, self.cut]
            recv = (recv1, recv2, recv3)[stage - 1].at[self.s, rows_, self.cut]
            return self.copy(stage - 1, send, recv, (self.n1, self.n2, self.n3)[stage - 1])

        def window(self, row, size):
            return y_ref.at[pl.ds(pl.multiple_of(row, 16), size), self.cols]

        def final(self):
            return final.at[self.k, pl.ds(0, self.size // 8), self.cut]

        def local(self):
            return pltpu.make_async_copy(
                self.final(), self.window(self.r3, self.size // 8), local_sem.at[self.p, self.s]
            )

        def gather(self, stage):
            if stage == 1:
                return self.copy(3, self.final(), self.window(self.r3, self.size // 8), self.n3)
            if stage == 2:
                w, device = self.window(self.r2, self.size // 4), self.n2
            else:
                w, device = self.window(self.r1, self.size // 2), self.n1
            return self.copy(stage + 2, w, w, device)

    def each_part(do):
        def stage(g, size, row):
            for p in range(len(parts)):
                do(Part(g, size, row, p))

        return stage

    def rows_at(offset, size):
        return pl.ds(pl.multiple_of(offset, 16), size)

    @each_part
    def sum1(q):
        h = q.size // 2
        send1[q.k, 0:h, q.cut] = part[q.k, rows_at((1 - q.b1) * h, h), q.cut].astype(jnp.bfloat16)
        q.reduce(1).start()

    @each_part
    def sum2(q):
        h = q.size // 4
        q.reduce(1).wait()
        for keep in (False, True):
            at = (q.b2 if keep else 1 - q.b2) * h
            total = part[q.k, rows_at(q.b1 * (q.size // 2) + at, h), q.cut] + recv1[
                q.s, rows_at(at, h), q.cut
            ].astype(jnp.float32)
            if keep:
                keep2[q.k, 0:h, q.cut] = total
            else:
                send2[q.k, 0:h, q.cut] = total.astype(jnp.bfloat16)
                q.reduce(2).start()

    @each_part
    def sum3(q):
        h = q.size // 8
        q.reduce(2).wait()
        for keep in (False, True):
            at = (q.b3 if keep else 1 - q.b3) * h
            total = keep2[q.k, rows_at(at, h), q.cut] + recv2[q.s, rows_at(at, h), q.cut].astype(jnp.float32)
            if keep:
                keep3[q.k, 0:h, q.cut] = total
            else:
                send3[q.k, 0:h, q.cut] = total.astype(jnp.bfloat16)
                q.reduce(3).start()

    @each_part
    def gather1(q):
        h = q.size // 8
        q.reduce(3).wait()
        total = keep3[q.k, 0:h, q.cut] + recv3[q.s, 0:h, q.cut].astype(jnp.float32)
        final[q.k, 0:h, q.cut] = total.astype(jnp.bfloat16)
        q.gather(1).start()
        q.local().start()

    @each_part
    def gather2(q):
        q.gather(1).wait()
        q.local().wait()
        q.gather(2).start()

    @each_part
    def gather3(q):
        q.gather(2).wait()
        q.gather(3).start()

    @each_part
    def gathered(q):
        q.gather(3).wait()

    def across(g, size, row):
        cols = pl.ds(pl.multiple_of(core * half + lax.rem(g, TILES) * group, group), group)
        w = y_ref.at[pl.ds(pl.multiple_of(row, 16), size), cols]
        return remote(w, w, core_send.at[g], core_recv.at[g], partner)

    def gather_core(g, size, row):
        gathered(g, size, row)
        across(g, size, row).start()

    def gather_core_wait(g, size, row):
        across(g, size, row).wait()

    stages = dict(
        sum2=sum2, sum3=sum3, gather1=gather1, gather2=gather2, gather3=gather3,
        gather_core=gather_core, gather_core_wait=gather_core_wait,
    )

    def events(i, place):
        for name, delay, where, first, last in EVENTS:
            if where == place:
                g = i - TILES - delay
                pl.when((g >= first) & (g < last))(
                    functools.partial(by_size, g // TILES, functools.partial(stages[name], g))
                )

    for pair in first_loads():
        for copy in pair:
            copy.start()
    load_up(0).start()

    def body(i, carry):
        slot, t = lax.rem(i // TILES, 2), lax.rem(i, TILES)
        g = i - TILES

        @pl.when(i + 1 < n)
        def _():
            load_gate(i + 1).start()
            load_up(i + 1).start()

        def activate(size, gate, up):
            hidden[slot, 0:size, columns(t, tile)] = (jax.nn.silu(gate) * up).astype(jnp.bfloat16)

        @pl.when(i == 0)
        def _():
            step, size = depth // SPLIT, SIZES[0]
            for k, pair in enumerate(first_loads()):
                for copy in pair:
                    copy.wait()
                cut = pl.ds(k * step, step)
                term = jnp.dot(xb[0, 0:size, cut], gb[0, cut], preferred_element_type=jnp.float32)
                gated[...] = term if k == 0 else gated[...] + term
            load_up(0).wait()
            activate(size, gated[...], jnp.dot(xb[0, 0:size], ub[0], preferred_element_type=jnp.float32))
            swap_down.start()
            if chunks > 1:
                start_x(1)

        @pl.when((i > 0) & (i < n))
        def _():
            load_gate(i).wait()
            load_up(i).wait()

            def dots(size, row):
                pl.when(t == 0)(lambda: load_x(i // TILES)(size, row).wait())
                gated[0:size] = jnp.dot(xb[slot, 0:size], gb[lax.rem(i, 2)], preferred_element_type=jnp.float32)
                up = jnp.dot(xb[slot, 0:size], ub[lax.rem(i, 2)], preferred_element_type=jnp.float32)
                activate(size, gated[0:size], up)

            by_size(i // TILES, dots)
            pl.when(t == TILES - 1)(lambda: start_x(i // TILES + 2))

        events(i, 0)
        pl.when(g == -1)(lambda: swap_down.wait())

        @pl.when((g >= -1) & (g < n - 1))
        def _():
            for copy in load_down(g + 1):
                copy.start()

        @pl.when((g >= 0) & (g < n))
        def _():
            for copy in load_down(g):
                copy.wait()

            def dot(size, row):
                @pl.when(lax.rem(g, TILES) == 0)
                def _():
                    for t in range(TILES):
                        swap_hidden((g // TILES) * TILES + t, size).wait()

                part[lax.rem(g, KEEP), 0:size] = jnp.dot(
                    hidden[lax.rem(g // TILES, 2), 0:size], db[lax.rem(g, 2)], preferred_element_type=jnp.float32
                )
                sum1(g, size, row)

            by_size(g // TILES, dot)

        pl.when(i < n)(lambda: by_size(i // TILES, lambda size, row: swap_hidden(i, size).start()))
        events(i, 1)
        return carry

    lax.fori_loop(0, n + TILES + 1 + max(e[1] for e in EVENTS), body, 0)


def block(x, w_gate, w_up, w_down):
    rows, depth = x.shape
    width = w_gate.shape[1]
    half = depth // 2
    tile, group, most = width // TILES, half // TILES, max(SIZES)
    b16, f32 = jnp.bfloat16, jnp.float32
    dma = pltpu.SemaphoreType.DMA
    flops = 6 * rows * depth * width
    y, _ = pl.pallas_call(
        kernel,
        out_shape=(jax.ShapeDtypeStruct((rows, depth), b16), jax.ShapeDtypeStruct((width, half), b16)),
        in_specs=[pl.BlockSpec(memory_space=pl.ANY)] * 4,
        out_specs=(pl.BlockSpec(memory_space=pl.ANY),) * 2,
        scratch_shapes=[
            pltpu.VMEM((2, most, depth), b16),
            pltpu.VMEM((2, depth, tile), b16),
            pltpu.VMEM((2, depth, tile), b16),
            pltpu.VMEM((2, 2 * width, group), b16),
            pltpu.VMEM((2, most, 2 * width), b16),
            pltpu.VMEM((most, tile), f32),
            pltpu.VMEM((KEEP, most, group), f32),
            pltpu.VMEM((KEEP, most // 2, group), b16),
            pltpu.VMEM((KEEP, most // 4, group), f32),
            pltpu.VMEM((KEEP, most // 4, group), b16),
            pltpu.VMEM((KEEP, most // 8, group), f32),
            pltpu.VMEM((KEEP, most // 8, group), b16),
            pltpu.VMEM((KEEP, most // 8, group), b16),
            pltpu.VMEM((SLOTS, most // 2, group), b16),
            pltpu.VMEM((SLOTS, most // 4, group), b16),
            pltpu.VMEM((SLOTS, most // 8, group), b16),
            dma((2, 2)), dma((2, SPLIT)), dma((2,)), dma((2, 2)), dma((2, TILES)), dma((2, TILES)), dma, dma, dma((len(PARTS), SLOTS)),
            dma((6, len(PARTS), SLOTS)), dma((6, len(PARTS), SLOTS)), dma((len(SIZES) * TILES,)), dma((len(SIZES) * TILES,)),
        ],
        compiler_params=pltpu.CompilerParams(
            collective_id=0, has_side_effects=True, vmem_limit_bytes=67_000_000
        ),
        cost_estimate=pl.CostEstimate(flops=flops, bytes_accessed=8 * depth * width, transcendentals=rows * width),
    )(x, w_gate, w_up, w_down)
    return y


def solution(mesh):
    return jax.shard_map(
        block,
        mesh=mesh,
        in_specs=(P("dp", None), P(None, "tp"), P(None, "tp"), P("tp", None)),
        out_specs=P("dp", None),
        check_vma=False,
    )
```
